16 devices in a mesh: dp: 2 (over y, z), stage: 8 (over x, core).
Axes of the slice: x: 4, y: 2, z: 1, core: 2. Of those that a mesh axis runs over, the one named last changes fastest.
The devices are a block of a 4x4x8 slice.
Arguments:
- token_ids: int32 [64, 128], P('dp'), parts along dimension 0
- label_ids: int32 [64, 128], P('dp'), parts along dimension 0
- embedding: bfloat16 [49152, 576], P('stage')
- w_in: bfloat16 [8, 576, 1536], P('stage')
- w_out: bfloat16 [8, 1536, 576], P('stage')
Outputs:
- output 1: float32 [2], P('dp'), parts along dimension 0
- output 2: float32 [16, 576, 1536], P(('dp', 'stage')), parts along dimension 0
- output 3: float32 [16, 1536, 576], P(('dp', 'stage')), parts along dimension 0
- output 4: float32 [98304, 576], P(('dp', 'stage')), parts along dimension 0
There are 2 independent parts. The reference program is written for one: setup_inputs(seed, part) draws one part's arguments, and reference() takes and returns one part's arrays. A program takes and returns all parts, laid end to end along the dimension named above; an argument that names none is the same for every part.
All inputs are finite; a program needn't handle non-finite values.
Results may differ from the reference program's by a relative error of at most 0.0144882.
Values are sent between devices in bfloat16 or wider.
A program may use at most 768 MiB of HBM per device.

```python
import functools
import jax
import jax.numpy as jnp
from jax import lax

VOCAB_SIZE = 49152
MODEL_DIM = 576
FFN_DIM = 1536
STAGES = 8
MICROBATCHES = 32
MICRO_TOKENS = 128
HOT_IDS = 64
NORM_EPS = 1e-6


def draw_ids(hot_ids, id_key):
    key_pick, key_unif, key_mix = jax.random.split(id_key, 3)
    shape_ids = (MICROBATCHES, MICRO_TOKENS)
    picked = hot_ids[jax.random.randint(key_pick, shape_ids, 0, HOT_IDS)]
    uniform_ids = jax.random.randint(key_unif, shape_ids, 0, VOCAB_SIZE)
    use_hot = jax.random.randint(key_mix, shape_ids, 0, 2) == 1
    return jnp.where(use_hot, picked, uniform_ids).astype(jnp.int32)


def setup_inputs(seed: int = 0, part: int = 0) -> dict:
    root_key = jax.random.key(seed)
    key_ids, key_emb, key_in, key_out = jax.random.split(root_key, 4)
    part_key = jax.random.fold_in(key_ids, part)
    key_hot, key_tok, key_lab = jax.random.split(part_key, 3)
    hot_ids = jax.random.randint(key_hot, (HOT_IDS,), 0, VOCAB_SIZE)
    token_ids = draw_ids(hot_ids, key_tok)
    label_ids = draw_ids(hot_ids, key_lab)
    embedding = jax.random.normal(key_emb, (VOCAB_SIZE, MODEL_DIM), jnp.float32).astype(jnp.bfloat16)
    w_in = (jax.random.normal(key_in, (STAGES, MODEL_DIM, FFN_DIM), jnp.float32) * MODEL_DIM ** -0.5).astype(jnp.bfloat16)
    w_out = (jax.random.normal(key_out, (STAGES, FFN_DIM, MODEL_DIM), jnp.float32) * 2.0 * (FFN_DIM * STAGES) ** -0.5).astype(jnp.bfloat16)
    return {"token_ids": token_ids, "label_ids": label_ids, "embedding": embedding, "w_in": w_in, "w_out": w_out}


def rms_normed(act_rows):
    acts_f = act_rows.astype(jnp.float32)
    return (acts_f * lax.rsqrt(jnp.mean(acts_f * acts_f, axis=-1, keepdims=True) + NORM_EPS)).astype(jnp.bfloat16)


def summed_loss(emb_f32, w_in_f32, w_out_f32, token_ids, label_ids):
    logit_scale = MODEL_DIM ** -0.5
    vocab_iota = jnp.arange(VOCAB_SIZE, dtype=jnp.int32)

    def layer_step(act_rows, weights):
        w_first, w_second = weights
        acts_f = act_rows.astype(jnp.float32)
        pre_act = jnp.dot(acts_f, w_first, preferred_element_type=jnp.float32)
        hidden = jax.nn.gelu(pre_act).astype(jnp.bfloat16)
        out_f = acts_f + jnp.dot(hidden.astype(jnp.float32), w_second, preferred_element_type=jnp.float32)
        return out_f.astype(jnp.bfloat16), None

    def micro_step(loss_total, ids_pair):
        tok_row, lab_row = ids_pair
        act_rows = emb_f32[tok_row].astype(jnp.bfloat16)
        act_rows, _ = lax.scan(layer_step, act_rows, (w_in_f32, w_out_f32))
        normed = rms_normed(act_rows).astype(jnp.float32)
        logits = jnp.dot(normed, emb_f32.T, preferred_element_type=jnp.float32) * logit_scale
        picked = jnp.sum(jnp.where(lab_row[:, None] == vocab_iota[None, :], logits, 0.0), axis=1)
        return loss_total + jnp.sum(jax.nn.logsumexp(logits, axis=1) - picked), None

    loss_total, _ = lax.scan(jax.checkpoint(micro_step), jnp.zeros((), jnp.float32), (token_ids, label_ids))
    return loss_total


def reference(token_ids, label_ids, embedding, w_in, w_out):
    loss_fn = functools.partial(summed_loss, token_ids=token_ids, label_ids=label_ids)
    loss_total, pull_back = jax.vjp(loss_fn, embedding.astype(jnp.float32), w_in.astype(jnp.float32), w_out.astype(jnp.float32))
    grad_emb, grad_in, grad_out = pull_back(jnp.ones((), jnp.float32))
    mean_loss = (loss_total / (MICROBATCHES * MICRO_TOKENS)).reshape(1)
    return (mean_loss, grad_in, grad_out, grad_emb)
```

```python
import functools

import jax
import jax.numpy as jnp
from jax import lax
from jax.experimental import pallas as pl
from jax.experimental.pallas import tpu as pltpu
from jax.sharding import PartitionSpec as P

NORM_EPS = 1e-6
MESH = pl.DeviceIdType.MESH
VMEM_BYTES = 66_000_000
FWD_ROWS = 128
BWD_ROWS = 256
HEAD_ROWS = 512
HEAD_COLS = 1024
SCATTER_ROWS = 512
GELU_K = 0.7978845608028654
GELU_C = 0.044715


def full_vmem():
    return pl.BlockSpec(memory_space=pltpu.VMEM)


def any_space():
    return pl.BlockSpec(memory_space=pl.ANY)


def remote(src, dst, send_sem, recv_sem, dev):
    return pltpu.make_async_remote_copy(
        src_ref=src, dst_ref=dst, send_sem=send_sem, recv_sem=recv_sem, device_id={"stage": dev}, device_id_type=MESH
    )


def group_barrier(me, n):
    barrier = pltpu.get_barrier_semaphore()
    for step in range(1, n):
        pl.semaphore_signal(barrier, inc=1, device_id={"stage": lax.rem(me + step, n)}, device_id_type=MESH)
    pl.semaphore_wait(barrier, n - 1)


def dot_nt(a, b):
    return lax.dot_general(a, b, (((1,), (1,)), ((), ())), preferred_element_type=jnp.float32)


def dot_tn(a, b):
    return lax.dot_general(a, b, (((0,), (0,)), ((), ())), preferred_element_type=jnp.float32)


def fwd_kernel(
    n, rows, w1, w2, xin_out, xl_out, h_out, dg_out,
    xin, xl, ea, eb, ec, es, y, hb, gb,
    e_send, ea_recv, eb_recv, ec_recv, f_send, x_recv, b_send, b_recv, h_sem, g_sem, o_sem,
):
    me = lax.axis_index("stage")
    size = FWD_ROWS
    count = rows.shape[0] // size
    last = n - 1
    odd = lax.rem(me, 2) == 1
    relay = odd & (me < last)
    group_barrier(me, n)

    def sl(c):
        return pl.ds(pl.multiple_of(c * size, size), size)

    def odd_send(c):
        return remote(rows.at[sl(c)], ea.at[sl(c)], e_send.at[c], ea_recv.at[c], me - 1)

    def even_send(c, dst, recv, dev):
        return remote(es.at[sl(c)], dst.at[sl(c)], e_send.at[c], recv.at[c], dev)

    def combine_and_send(c, has_eb, dst, recv, dev):
        even_send(c, ea, ea_recv, me).wait_recv()
        total = rows[sl(c), :] + ea[sl(c), :]
        if has_eb:
            even_send(c, eb, eb_recv, me).wait_recv()
            total = total + eb[sl(c), :]
        es[sl(c), :] = total
        even_send(c, dst, recv, dev).start()

    lead = 6

    @pl.when(odd)
    def _():
        @pl.loop(0, count)
        def _(c):
            odd_send(c).start()

    @pl.when(me == 4)
    def _():
        @pl.loop(0, count)
        def _(c):
            combine_and_send(c, False, eb, eb_recv, 2)

    @pl.when(me == 6)
    def _():
        @pl.loop(0, count)
        def _(c):
            combine_and_send(c, False, ec, ec_recv, 0)

    @pl.when(me == 2)
    def _():
        @pl.loop(0, lead)
        def _(c):
            combine_and_send(c, True, eb, eb_recv, 0)

    def fwd_send(c):
        return remote(y.at[sl(c)], xin.at[sl(c)], f_send.at[c], x_recv.at[c], me + 1)

    def bcast(src, c, which, dev):
        return remote(src.at[sl(c)], xl.at[sl(c)], b_send.at[which, c], b_recv.at[c], dev)

    def h_copy(c, slot):
        return pltpu.make_async_copy(hb.at[slot], h_out.at[sl(c)], h_sem.at[slot])

    def g_copy(c, slot):
        return pltpu.make_async_copy(gb.at[slot], dg_out.at[sl(c)], g_sem.at[slot])

    def layer(c):
        slot = lax.rem(c, 2)

        @pl.when(me == 0)
        def _():
            even_send(c, ea, ea_recv, me).wait_recv()
            even_send(c, eb, eb_recv, me).wait_recv()
            even_send(c, ec, ec_recv, me).wait_recv()
            xin[sl(c), :] = (rows[sl(c), :] + ea[sl(c), :]) + (eb[sl(c), :] + ec[sl(c), :])

        @pl.when(me > 0)
        def _():
            remote(y.at[sl(c)], xin.at[sl(c)], f_send.at[c], x_recv.at[c], me).wait_recv()

        @pl.when(c >= 2)
        def _():
            h_copy(c - 2, slot).wait()
            g_copy(c - 2, slot).wait()

        x = xin[sl(c), :]
        pre = jnp.dot(x, w1[...], preferred_element_type=jnp.float32)
        sq = pre * pre
        th = jnp.tanh(GELU_K * (pre + GELU_C * (pre * sq)))
        cdf = 0.5 * (1.0 + th)
        hidden = (pre * cdf).astype(jnp.bfloat16)
        gb[slot] = cdf + (0.5 * pre) * (1.0 - th * th) * (GELU_K + (3.0 * GELU_K * GELU_C) * sq)
        hb[slot] = hidden
        out = x.astype(jnp.float32) + jnp.dot(hidden, w2[...], preferred_element_type=jnp.float32)
        y[sl(c), :] = out.astype(jnp.bfloat16)

        @pl.when(me < last)
        def _():
            fwd_send(c).start()

        @pl.when(me == last)
        def _():
            bcast(y, c, 0, last - 1).start()

            @pl.when(lax.rem(c, 2) == 0)
            def _():
                bcast(y, c, 1, 1).start()

            @pl.when(lax.rem(c, 2) == 1)
            def _():
                bcast(y, c, 1, last - 2).start()

        h_copy(c, slot).start()
        g_copy(c, slot).start()

    def has_next(c):
        up = lax.rem(c, 2) == 0
        return (up & (me < last - 2)) | (jnp.logical_not(up) & (me > 1))

    def next_relay(c):
        return me + 2 - 4 * lax.rem(c, 2)

    def relay_step(c):
        bcast(xl, c, 0, me).wait_recv()
        bcast(xl, c, 0, me - 1).start()

        @pl.when(has_next(c))
        def _():
            bcast(xl, c, 1, next_relay(c)).start()

    lag = (last - me) * 2 + 4

    @pl.loop(0, count + 2 * last + 4)
    def _(i):
        @pl.when((me == 2) & (i + lead < count))
        def _():
            combine_and_send(i + lead, True, eb, eb_recv, 0)

        @pl.when(i < count)
        def _():
            layer(i)

        @pl.when(relay & (i >= lag) & (i - lag < count))
        def _():
            relay_step(i - lag)

    @pl.when(jnp.logical_not(odd))
    def _():
        @pl.loop(0, count)
        def _(c):
            bcast(xl, c, 0, me).wait_recv()

    @pl.when(me == last)
    def _():
        xl[...] = y[...]

    copy_xin = pltpu.make_async_copy(xin, xin_out, o_sem.at[0])
    copy_xl = pltpu.make_async_copy(xl, xl_out, o_sem.at[1])
    copy_xin.start()
    copy_xl.start()

    @pl.loop(0, count)
    def _(c):
        @pl.when(odd)
        def _():
            odd_send(c).wait_send()

        @pl.when(jnp.logical_not(odd) & (me > 0))
        def _():
            even_send(c, eb, eb_recv, me).wait_send()

        @pl.when(me < last)
        def _():
            fwd_send(c).wait_send()

        @pl.when(odd)
        def _():
            bcast(xl, c, 0, me).wait_send()

        @pl.when((me == last) | (relay & has_next(c)))
        def _():
            bcast(xl, c, 1, me).wait_send()

    for c in (count - 2, count - 1):
        h_copy(c, c % 2).wait()
        g_copy(c, c % 2).wait()
    copy_xin.wait()
    copy_xl.wait()


def head_kernel(
    n, xl, emb, lab, det, gl, loss,
    nblk, ntr, probs, mt, st, labsum, cmat, gn, gsend, gr, gst, sstat, rstat,
    s_send, s_recv, g_send, g_recv, l_send, l_recv,
):
    me = lax.axis_index("stage")
    last = n - 1
    tokens, dim = xl.shape
    slice_rows = emb.shape[0]
    size, cols = HEAD_ROWS, HEAD_COLS
    blocks, tiles = tokens // size, slice_rows // cols
    own = size // n
    scale = dim ** -0.5
    group_barrier(me, n)
    lane = lax.broadcasted_iota(jnp.int32, (size, 128), 1)

    def sl(b):
        return pl.ds(pl.multiple_of(b * size, size), size)

    def tile(j):
        return pl.ds(pl.multiple_of(j * cols, cols), cols)

    def own_rows(b, dev):
        return pl.ds(pl.multiple_of(b * size + dev * own, own), own)

    def peer(step):
        return lax.rem(me + step, n)

    def stat_send(b, dev):
        return remote(sstat.at[b], rstat.at[b, me], s_send.at[b, dev], s_recv.at[b, me], dev)

    def stat_recv(b, dev):
        return remote(sstat.at[b], rstat.at[b, dev], s_send.at[b, dev], s_recv.at[b, dev], me)

    def grad_piece(b, dev):
        return gsend.at[lax.rem(b, 2), pl.ds(pl.multiple_of(dev * own, own), own)]

    def grad_send(b, dev):
        return remote(grad_piece(b, dev), gr.at[b, me], g_send.at[b, dev], g_recv.at[b, me], dev)

    def grad_recv(b, dev):
        return remote(grad_piece(b, dev), gr.at[b, dev], g_send.at[b, dev], g_recv.at[b, dev], me)

    def last_send(b):
        return remote(gst.at[b], gl.at[own_rows(b, me)], l_send.at[b], l_recv.at[b, me], last)

    def last_recv(b, dev):
        return remote(gst.at[b], gl.at[own_rows(b, dev)], l_send.at[b], l_recv.at[b, dev], me)

    def last_copy(b):
        return pltpu.make_async_copy(gst.at[b], gl.at[own_rows(b, me)], l_send.at[b])

    def label_mask(b, j):
        ids = lax.broadcasted_iota(jnp.int32, (size, cols), 1)
        return ids == (lab[sl(b), :] - j * cols)

    def open_block(b):
        acts = xl[sl(b), :].astype(jnp.float32)
        normed = acts * lax.rsqrt(jnp.mean(acts * acts, axis=-1, keepdims=True) + NORM_EPS)
        nblk[...] = normed.astype(jnp.bfloat16)
        ntr[lax.rem(b, 3)] = normed.T.astype(jnp.bfloat16)
        mt[lax.rem(b, 3)] = jnp.full((size, 128), -jnp.inf, jnp.float32)
        st[...] = jnp.zeros((size, 128), jnp.float32)
        labsum[...] = jnp.zeros((size, 128), jnp.float32)

    def logits_tile(b, j):
        logits = dot_nt(nblk[...], emb[tile(j), :])
        row_max = jnp.max(logits, axis=1, keepdims=True)
        exps = jnp.exp((logits - row_max) * scale)
        probs[lax.rem(b, 2), :, tile(j)] = exps.astype(jnp.bfloat16)
        here = lane == j
        mt[lax.rem(b, 3)] = jnp.where(here, row_max, mt[lax.rem(b, 3)])
        st[...] = jnp.where(here, jnp.sum(exps, axis=1, keepdims=True), st[...])
        labsum[...] += jnp.sum(jnp.where(label_mask(b, j), logits, 0.0), axis=1, keepdims=True)

    def close_block(b):
        tile_max = mt[lax.rem(b, 3)]
        row_max = jnp.max(tile_max, axis=1, keepdims=True)
        row_sum = jnp.sum(st[...] * jnp.exp((tile_max - row_max) * scale), axis=1, keepdims=True)
        packed = jnp.where(lane == 0, row_max, jnp.where(lane == 1, row_sum, labsum[...]))
        rows = packed.T[:8]
        sstat[b] = rows
        rstat[b, me] = rows
        for step in range(1, n):
            stat_send(b, peer(step)).start()

    def join_stats(b):
        for step in range(1, n):
            stat_recv(b, peer(step)).wait_recv()
        parts = [rstat[b, dev] for dev in range(n)]
        row_max = functools.reduce(jnp.maximum, [part[0:1] for part in parts])
        row_sum = sum(part[1:2] * jnp.exp((part[0:1] - row_max) * scale) for part in parts)
        row_lab = sum(part[2:3] for part in parts)
        lse = row_max * scale + jnp.log(row_sum)
        loss[...] += jnp.sum(lse - row_lab * scale)
        lse_cols = jnp.broadcast_to(lse, (128, size)).T
        cmat[...] = jnp.exp(mt[lax.rem(b, 3)] * scale - lse_cols) * scale
        gn[...] = jnp.zeros_like(gn)

    def grad_tile(b, j):
        factor = jnp.sum(jnp.where(lane == j, cmat[...], 0.0), axis=1, keepdims=True)
        exps = probs[lax.rem(b, 2), :, tile(j)].astype(jnp.float32)
        dlog = (exps * factor - jnp.where(label_mask(b, j), scale, 0.0)).astype(jnp.bfloat16)
        gn[...] += jnp.dot(dlog, emb[tile(j), :], preferred_element_type=jnp.float32)
        det[:, tile(j)] += jnp.dot(ntr[lax.rem(b, 3)], dlog, preferred_element_type=jnp.float32)

    def wait_grad_sends(b):
        for step in range(1, n):
            grad_send(b, peer(step)).wait_send()

    def send_grads(b):
        if isinstance(b, int):
            if b >= 2:
                wait_grad_sends(b - 2)
        else:
            @pl.when(b >= 2)
            def _():
                wait_grad_sends(b - 2)
        gsend[lax.rem(b, 2)] = gn[...].astype(jnp.bfloat16)
        gr[b, me] = gn[pl.ds(pl.multiple_of(me * own, own), own), :].astype(jnp.bfloat16)
        for step in range(1, n):
            grad_send(b, peer(step)).start()

    def own_block(b):
        for step in range(1, n):
            grad_recv(b, peer(step)).wait_recv()
        grad = sum(gr[b, dev].astype(jnp.float32) for dev in range(n))
        acts = xl[own_rows(b, me), :].astype(jnp.float32)
        inv = lax.rsqrt(jnp.mean(acts * acts, axis=-1, keepdims=True) + NORM_EPS)
        normed = acts * inv
        out = inv * (grad - normed * jnp.mean(grad * normed, axis=-1, keepdims=True))
        gst[b] = out.astype(jnp.bfloat16)

        @pl.when(me < last)
        def _():
            last_send(b).start()

        @pl.when(me == last)
        def _():
            last_copy(b).start()

    det[...] = jnp.zeros_like(det)
    loss[...] = jnp.zeros_like(loss)

    @pl.loop(0, 2)
    def _(b):
        open_block(b)

        @pl.loop(0, tiles)
        def _(j):
            logits_tile(b, j)

        close_block(b)

    @pl.loop(2, blocks)
    def _(b):
        join_stats(b - 2)
        open_block(b)

        @pl.loop(0, tiles)
        def _(j):
            grad_tile(b - 2, j)
            logits_tile(b, j)

        close_block(b)

        @pl.when(b >= 3)
        def _():
            own_block(b - 3)

        send_grads(b - 2)

    @pl.loop(blocks - 2, blocks)
    def _(b):
        join_stats(b)

        @pl.loop(0, tiles)
        def _(j):
            grad_tile(b, j)

        own_block(b - 1)
        send_grads(b)

    own_block(blocks - 1)

    @pl.loop(0, blocks)
    def _(b):
        for step in range(1, n):
            stat_send(b, peer(step)).wait_send()

        @pl.when(b >= blocks - 2)
        def _():
            wait_grad_sends(b)

        @pl.when(me < last)
        def _():
            last_send(b).wait_send()

        @pl.when(me == last)
        def _():
            last_copy(b).wait()
            for dev in range(n - 1):
                last_recv(b, dev).wait_recv()


def bwd_kernel(
    n, gl, xin, h_in, dg_in, w1, w2, dw1, dw2t, gx_out,
    gin, gout, gall, hb, gb,
    f_send, g_recv, b_send, b_recv, h_sem, d_sem, o_sem,
):
    me = lax.axis_index("stage")
    last = n - 1
    size = BWD_ROWS
    count = xin.shape[0] // size
    odd = lax.rem(me, 2) == 1
    relay = jnp.logical_not(odd) & (me > 0)
    group_barrier(me, n)

    def sl(c):
        return pl.ds(pl.multiple_of(c * size, size), size)

    def h_copy(c):
        slot = lax.rem(c, 2)
        return pltpu.make_async_copy(h_in.at[sl(c)], hb.at[slot], h_sem.at[slot])

    def d_copy(c):
        slot = lax.rem(c, 2)
        return pltpu.make_async_copy(dg_in.at[sl(c)], gb.at[slot], d_sem.at[slot])

    def grad_send(c, dev):
        return remote(gout.at[sl(c)], gin.at[sl(c)], f_send.at[c], g_recv.at[c], dev)

    def bcast(src, c, which, dev):
        return remote(src.at[sl(c)], gall.at[sl(c)], b_send.at[which, c], b_recv.at[c], dev)

    h_copy(0).start()
    d_copy(0).start()
    dw1[...] = jnp.zeros_like(dw1)
    dw2t[...] = jnp.zeros_like(dw2t)

    @pl.when(me == last)
    def _():
        whole = pltpu.make_async_copy(gl, gin, o_sem.at[0])
        whole.start()
        whole.wait()

    def layer(c):
        slot = lax.rem(c, 2)

        @pl.when(c + 1 < count)
        def _():
            h_copy(c + 1).start()
            d_copy(c + 1).start()

        h_copy(c).wait()
        d_copy(c).wait()

        @pl.when(me < last)
        def _():
            grad_send(c, me).wait_recv()

        grad = gin[sl(c), :]
        grad_hidden = dot_nt(grad, w2[...])
        grad_pre = (grad_hidden * gb[slot]).astype(jnp.bfloat16)
        grad_in = grad.astype(jnp.float32) + dot_nt(grad_pre, w1[...])
        gout[sl(c), :] = grad_in.astype(jnp.bfloat16)

        @pl.when(me > 0)
        def _():
            grad_send(c, me - 1).start()

        @pl.when(me == 0)
        def _():
            bcast(gout, c, 0, 1).start()
            bcast(gout, c, 1, 2).start()
            bcast(gout, c, 2, last - 1).start()

        dw1[...] += dot_tn(xin[sl(c), :], grad_pre)
        dw2t[...] += dot_tn(grad, hb[slot])

    def relay_step(c):
        bcast(gall, c, 0, me).wait_recv()
        bcast(gall, c, 0, me + 1).start()

        @pl.when(me == 2)
        def _():
            bcast(gall, c, 1, 4).start()

    lag = me + 2

    @pl.loop(0, count + n)
    def _(i):
        @pl.when(i < count)
        def _():
            layer(i)

        @pl.when(relay & (i >= lag) & (i - lag < count))
        def _():
            relay_step(i - lag)

    @pl.when(odd)
    def _():
        @pl.loop(0, count)
        def _(c):
            bcast(gall, c, 0, me).wait_recv()

    @pl.when(me == 0)
    def _():
        whole = pltpu.make_async_copy(gout, gx_out, o_sem.at[0])
        whole.start()
        whole.wait()

    @pl.when(me > 0)
    def _():
        whole = pltpu.make_async_copy(gall, gx_out, o_sem.at[0])
        whole.start()
        whole.wait()

    @pl.loop(0, count)
    def _(c):
        @pl.when(me > 0)
        def _():
            grad_send(c, me).wait_send()

        @pl.when(jnp.logical_not(odd))
        def _():
            bcast(gall, c, 0, me).wait_send()

        @pl.when((me == 0) | (me == 2))
        def _():
            bcast(gall, c, 1, me).wait_send()

        @pl.when(me == 0)
        def _():
            bcast(gall, c, 2, me).wait_send()


def scatter_kernel(starts, ids, pos, det, gx, out, grads):
    blk = pl.program_id(0)

    @pl.when(blk == 0)
    def _():
        grads[...] = gx[...].astype(jnp.float32)

    out[...] = det[...].T
    base = blk * SCATTER_ROWS

    def add_row(k, carry):
        row = pl.ds(ids[k] - base, 1)
        out[row, :] = out[row, :] + grads[pl.ds(pos[k], 1), :]
        return carry

    lax.fori_loop(starts[blk], starts[blk + 1], add_row, 0)


def comm_params(collective_id):
    return pltpu.CompilerParams(collective_id=collective_id, has_side_effects=True, vmem_limit_bytes=VMEM_BYTES)


def solution(mesh):
    n = mesh.shape["stage"]
    bf16, f32 = jnp.bfloat16, jnp.float32
    dma = pltpu.SemaphoreType.DMA
    shape = jax.ShapeDtypeStruct

    def stage_body(token_ids, label_ids, emb_rows, w_in, w_out):
        stage_idx = lax.axis_index("stage")
        micro_count, micro_tokens = token_ids.shape
        tokens = micro_count * micro_tokens
        slice_rows, dim = emb_rows.shape
        w1, w2 = w_in[0], w_out[0]
        ffn = w1.shape[1]
        row_start = stage_idx * slice_rows

        local_tok = token_ids.reshape(tokens) - row_start
        tok_here = (local_tok >= 0) & (local_tok < slice_rows)
        looked_up = jnp.take(emb_rows, jnp.clip(local_tok, 0, slice_rows - 1), axis=0)
        rows = jnp.where(tok_here[:, None], looked_up, 0)
        local_lab = label_ids.reshape(tokens, 1) - row_start

        keys = jnp.where(tok_here, local_tok, slice_rows)
        sorted_ids, sorted_pos = lax.sort((keys, lax.iota(jnp.int32, tokens)), num_keys=1, is_stable=False)
        edges = lax.iota(jnp.int32, slice_rows // SCATTER_ROWS + 1) * SCATTER_ROWS
        starts = jnp.sum((keys[None, :] < edges[:, None]).astype(jnp.int32), axis=1)

        size, count = FWD_ROWS, tokens // FWD_ROWS
        big = pltpu.VMEM((tokens, dim), bf16)
        xin, xl, hidden, dgelu = pl.pallas_call(
            functools.partial(fwd_kernel, n),
            name="forward",
            out_shape=[shape((tokens, dim), bf16), shape((tokens, dim), bf16), shape((tokens, ffn), bf16), shape((tokens, ffn), f32)],
            in_specs=[full_vmem()] * 3,
            out_specs=[any_space()] * 4,
            scratch_shapes=[big] * 7
            + [pltpu.VMEM((2, size, ffn), bf16), pltpu.VMEM((2, size, ffn), f32)]
            + [dma((count,))] * 6
            + [dma((2, count)), dma((count,)), dma((2,)), dma((2,)), dma((2,))],
            compiler_params=comm_params(1),
        )(rows, w1, w2)

        blocks = tokens // HEAD_ROWS
        own = HEAD_ROWS // n
        stat = pltpu.VMEM((HEAD_ROWS, 128), f32)
        det, gl, loss = pl.pallas_call(
            functools.partial(head_kernel, n),
            name="head",
            out_shape=[shape((dim, slice_rows), f32), shape((tokens, dim), bf16), shape((8, 128), f32)],
            in_specs=[full_vmem()] * 3,
            out_specs=[full_vmem(), any_space(), full_vmem()],
            scratch_shapes=[
                pltpu.VMEM((HEAD_ROWS, dim), bf16),
                pltpu.VMEM((3, dim, HEAD_ROWS), bf16),
                pltpu.VMEM((2, HEAD_ROWS, slice_rows), bf16),
                pltpu.VMEM((3, HEAD_ROWS, 128), f32),
                stat, stat, stat,
                pltpu.VMEM((HEAD_ROWS, dim), f32),
                pltpu.VMEM((2, HEAD_ROWS, dim), bf16),
                pltpu.VMEM((blocks, n, own, dim), bf16),
                pltpu.VMEM((blocks, own, dim), bf16),
                pltpu.VMEM((blocks, 8, HEAD_ROWS), f32),
                pltpu.VMEM((blocks, n, 8, HEAD_ROWS), f32),
            ]
            + [dma((blocks, n))] * 4
            + [dma((blocks,)), dma((blocks, n))],
            compiler_params=comm_params(2),
        )(xl, emb_rows, local_lab)

        size, count = BWD_ROWS, tokens // BWD_ROWS
        dw1, dw2t, gx = pl.pallas_call(
            functools.partial(bwd_kernel, n),
            name="backward",
            out_shape=[shape((dim, ffn), f32), shape((dim, ffn), f32), shape((tokens, dim), bf16)],
            in_specs=[any_space(), full_vmem(), any_space(), any_space(), full_vmem(), full_vmem()],
            out_specs=[full_vmem(), full_vmem(), any_space()],
            scratch_shapes=[big] * 3
            + [pltpu.VMEM((2, size, ffn), bf16), pltpu.VMEM((2, size, ffn), f32)]
            + [dma((count,))] * 2
            + [dma((3, count)), dma((count,)), dma((2,)), dma((2,)), dma((1,))],
            compiler_params=comm_params(3),
        )(gl, xin, hidden, dgelu, w1, w2)

        smem = pl.BlockSpec(memory_space=pltpu.SMEM)
        grad_emb = pl.pallas_call(
            scatter_kernel,
            name="lookup_grad",
            grid=(slice_rows // SCATTER_ROWS,),
            out_shape=shape((slice_rows, dim), f32),
            in_specs=[smem, smem, smem, pl.BlockSpec((dim, SCATTER_ROWS), lambda i: (0, i)), full_vmem()],
            out_specs=pl.BlockSpec((SCATTER_ROWS, dim), lambda i: (i, 0)),
            scratch_shapes=[pltpu.VMEM((tokens, dim), f32)],
            compiler_params=pltpu.CompilerParams(dimension_semantics=("arbitrary",), vmem_limit_bytes=VMEM_BYTES),
        )(starts, sorted_ids, sorted_pos, det, gx)

        mean_loss = (loss[0, :1] / tokens).astype(f32)
        return mean_loss, dw1[None], dw2t.T[None], grad_emb

    return jax.shard_map(
        stage_body,
        mesh=mesh,
        in_specs=(P("dp", None), P("dp", None), P("stage", None), P("stage", None, None), P("stage", None, None)),
        out_specs=(P("dp"), P(("dp", "stage"), None, None), P(("dp", "stage"), None, None), P(("dp", "stage"), None)),
        check_vma=False,
    )
```

```python
import functools

import jax
import jax.numpy as jnp
from jax import lax
from jax.experimental import pallas as pl
from jax.experimental.pallas import tpu as pltpu
from jax.sharding import PartitionSpec as P

NORM_EPS = 1e-6
MESH = pl.DeviceIdType.MESH
VMEM_BYTES = 66_000_000
FWD_ROWS = 128
BWD_ROWS = 256
HEAD_ROWS = 512
HEAD_COLS = 2048
SCATTER_ROWS = 512
GELU_K = 0.7978845608028654
GELU_C = 0.044715


def full_vmem():
    return pl.BlockSpec(memory_space=pltpu.VMEM)


def any_space():
    return pl.BlockSpec(memory_space=pl.ANY)


def remote(src, dst, send_sem, recv_sem, dev):
    return pltpu.make_async_remote_copy(
        src_ref=src, dst_ref=dst, send_sem=send_sem, recv_sem=recv_sem, device_id={"stage": dev}, device_id_type=MESH
    )


def group_barrier(me, n):
    barrier = pltpu.get_barrier_semaphore()
    for step in range(1, n):
        pl.semaphore_signal(barrier, inc=1, device_id={"stage": lax.rem(me + step, n)}, device_id_type=MESH)
    pl.semaphore_wait(barrier, n - 1)


def dot_nt(a, b):
    return lax.dot_general(a, b, (((1,), (1,)), ((), ())), preferred_element_type=jnp.float32)


def dot_tn(a, b):
    return lax.dot_general(a, b, (((0,), (0,)), ((), ())), preferred_element_type=jnp.float32)


def fwd_kernel(
    n, rows, w1, w2, xin_out, xl_out, h_out, dg_out,
    xin, xl, ea, eb, ec, es, y, hb, gb,
    e_send, ea_recv, eb_recv, ec_recv, f_send, x_recv, b_send, b_recv, h_sem, g_sem, o_sem,
):
    me = lax.axis_index("stage")
    size = FWD_ROWS
    count = rows.shape[0] // size
    last = n - 1
    odd = lax.rem(me, 2) == 1
    relay = odd & (me < last)
    group_barrier(me, n)

    def sl(c):
        return pl.ds(pl.multiple_of(c * size, size), size)

    def odd_send(c):
        return remote(rows.at[sl(c)], ea.at[sl(c)], e_send.at[c], ea_recv.at[c], me - 1)

    def even_send(c, dst, recv, dev):
        return remote(es.at[sl(c)], dst.at[sl(c)], e_send.at[c], recv.at[c], dev)

    def combine_and_send(c, has_eb, dst, recv, dev):
        even_send(c, ea, ea_recv, me).wait_recv()
        total = rows[sl(c), :] + ea[sl(c), :]
        if has_eb:
            even_send(c, eb, eb_recv, me).wait_recv()
            total = total + eb[sl(c), :]
        es[sl(c), :] = total
        even_send(c, dst, recv, dev).start()

    lead = 8

    @pl.when(odd)
    def _():
        @pl.loop(0, count)
        def _(c):
            odd_send(c).start()

    @pl.when(me == 4)
    def _():
        @pl.loop(0, count)
        def _(c):
            combine_and_send(c, False, eb, eb_recv, 2)

    @pl.when(me == 6)
    def _():
        @pl.loop(0, count)
        def _(c):
            combine_and_send(c, False, ec, ec_recv, 0)

    @pl.when(me == 2)
    def _():
        @pl.loop(0, lead)
        def _(c):
            combine_and_send(c, True, eb, eb_recv, 0)

    def fwd_send(c):
        return remote(y.at[sl(c)], xin.at[sl(c)], f_send.at[c], x_recv.at[c], me + 1)

    def bcast(src, c, which, dev):
        return remote(src.at[sl(c)], xl.at[sl(c)], b_send.at[which, c], b_recv.at[c], dev)

    def h_copy(c, slot):
        return pltpu.make_async_copy(hb.at[slot], h_out.at[sl(c)], h_sem.at[slot])

    def g_copy(c, slot):
        return pltpu.make_async_copy(gb.at[slot], dg_out.at[sl(c)], g_sem.at[slot])

    def layer(c):
        slot = lax.rem(c, 2)

        @pl.when(me == 0)
        def _():
            even_send(c, ea, ea_recv, me).wait_recv()
            even_send(c, eb, eb_recv, me).wait_recv()
            even_send(c, ec, ec_recv, me).wait_recv()
            xin[sl(c), :] = (rows[sl(c), :] + ea[sl(c), :]) + (eb[sl(c), :] + ec[sl(c), :])

        @pl.when(me > 0)
        def _():
            remote(y.at[sl(c)], xin.at[sl(c)], f_send.at[c], x_recv.at[c], me).wait_recv()

        @pl.when(c >= 2)
        def _():
            h_copy(c - 2, slot).wait()
            g_copy(c - 2, slot).wait()

        x = xin[sl(c), :]
        pre = jnp.dot(x, w1[...], preferred_element_type=jnp.float32)
        sq = pre * pre
        th = jnp.tanh(GELU_K * (pre + GELU_C * (pre * sq)))
        cdf = 0.5 * (1.0 + th)
        hidden = (pre * cdf).astype(jnp.bfloat16)
        gb[slot] = cdf + (0.5 * pre) * (1.0 - th * th) * (GELU_K + (3.0 * GELU_K * GELU_C) * sq)
        hb[slot] = hidden
        out = x.astype(jnp.float32) + dot_nt(hidden, w2[...])
        y[sl(c), :] = out.astype(jnp.bfloat16)

        @pl.when(me < last)
        def _():
            fwd_send(c).start()

        @pl.when(me == last)
        def _():
            bcast(y, c, 0, last - 1).start()

            bcast(y, c, 1, 1).start()
            bcast(y, c, 2, last - 2).start()

        h_copy(c, slot).start()
        g_copy(c, slot).start()

    def has_next(c):
        up = lax.rem(c, 2) == 0
        return (up & (me == 1)) | (jnp.logical_not(up) & (me == last - 2))

    def relay_step(c):
        bcast(xl, c, 0, me).wait_recv()
        bcast(xl, c, 0, me - 1).start()

        @pl.when(has_next(c))
        def _():
            bcast(xl, c, 1, 3).start()

    lag = jnp.where(me == 1, 24, jnp.where(me == 3, count, 14))

    @pl.loop(0, 2 * count)
    def _(i):
        @pl.when((me == 2) & (i + lead < count))
        def _():
            combine_and_send(i + lead, True, eb, eb_recv, 0)

        @pl.when(i < count)
        def _():
            layer(i)

        @pl.when(relay & (i >= lag) & (i - lag < count))
        def _():
            relay_step(i - lag)

    @pl.when(jnp.logical_not(odd))
    def _():
        @pl.loop(0, count)
        def _(c):
            bcast(xl, c, 0, me).wait_recv()

    @pl.when(me == last)
    def _():
        xl[...] = y[...]

    copy_xin = pltpu.make_async_copy(xin, xin_out, o_sem.at[0])
    copy_xl = pltpu.make_async_copy(xl, xl_out, o_sem.at[1])
    copy_xin.start()
    copy_xl.start()

    @pl.loop(0, count)
    def _(c):
        @pl.when(odd)
        def _():
            odd_send(c).wait_send()

        @pl.when(jnp.logical_not(odd) & (me > 0))
        def _():
            even_send(c, eb, eb_recv, me).wait_send()

        @pl.when(me < last)
        def _():
            fwd_send(c).wait_send()

        @pl.when(odd)
        def _():
            bcast(xl, c, 0, me).wait_send()

        @pl.when((me == last) | (relay & has_next(c)))
        def _():
            bcast(xl, c, 1, me).wait_send()

        @pl.when(me == last)
        def _():
            bcast(xl, c, 2, me).wait_send()

    for c in (count - 2, count - 1):
        h_copy(c, c % 2).wait()
        g_copy(c, c % 2).wait()
    copy_xin.wait()
    copy_xl.wait()


def head_kernel(
    n, xl, emb, lab, det, gl, loss,
    nblk, ntr, probs, mt, st, labsum, cmat, gn, gsend, gr, gst, sstat, rstat,
    s_send, s_recv, g_send, g_recv, l_send, l_recv,
):
    me = lax.axis_index("stage")
    last = n - 1
    tokens, dim = xl.shape
    slice_rows = emb.shape[1]
    size, cols = HEAD_ROWS, HEAD_COLS
    blocks, tiles = tokens // size, slice_rows // cols
    own = size // n
    scale = dim ** -0.5
    group_barrier(me, n)
    lane = lax.broadcasted_iota(jnp.int32, (size, 128), 1)

    def sl(b):
        return pl.ds(pl.multiple_of(b * size, size), size)

    def tile(j):
        return pl.ds(pl.multiple_of(j * cols, cols), cols)

    def own_rows(b, dev):
        return pl.ds(pl.multiple_of(b * size + dev * own, own), own)

    def peer(step):
        return lax.rem(me + step, n)

    def stat_send(b, dev):
        return remote(sstat.at[b], rstat.at[b, me], s_send.at[b, dev], s_recv.at[b, me], dev)

    def stat_recv(b, dev):
        return remote(sstat.at[b], rstat.at[b, dev], s_send.at[b, dev], s_recv.at[b, dev], me)

    def grad_piece(b, dev):
        return gsend.at[lax.rem(b, 2), pl.ds(pl.multiple_of(dev * own, own), own)]

    def grad_send(b, dev):
        return remote(grad_piece(b, dev), gr.at[b, me], g_send.at[b, dev], g_recv.at[b, me], dev)

    def grad_recv(b, dev):
        return remote(grad_piece(b, dev), gr.at[b, dev], g_send.at[b, dev], g_recv.at[b, dev], me)

    def last_send(b):
        return remote(gst.at[b], gl.at[own_rows(b, me)], l_send.at[b], l_recv.at[b, me], last)

    def last_recv(b, dev):
        return remote(gst.at[b], gl.at[own_rows(b, dev)], l_send.at[b], l_recv.at[b, dev], me)

    def last_copy(b):
        return pltpu.make_async_copy(gst.at[b], gl.at[own_rows(b, me)], l_send.at[b])

    def label_mask(b, j):
        ids = lax.broadcasted_iota(jnp.int32, (size, cols), 1)
        return ids == (lab[sl(b), :] - j * cols)

    def open_block(b):
        acts = xl[sl(b), :].astype(jnp.float32)
        normed = acts * lax.rsqrt(jnp.mean(acts * acts, axis=-1, keepdims=True) + NORM_EPS)
        nblk[...] = normed.astype(jnp.bfloat16)
        ntr[lax.rem(b, 3)] = normed.T.astype(jnp.bfloat16)
        mt[lax.rem(b, 3)] = jnp.full((size, 128), -jnp.inf, jnp.float32)
        st[...] = jnp.zeros((size, 128), jnp.float32)
        labsum[...] = jnp.zeros((size, 128), jnp.float32)

    def logits_tile(b, j):
        logits = jnp.dot(nblk[...], emb[:, tile(j)], preferred_element_type=jnp.float32)
        row_max = jnp.max(logits, axis=1, keepdims=True)
        exps = jnp.exp((logits - row_max) * scale)
        probs[lax.rem(b, 2), :, tile(j)] = exps.astype(jnp.bfloat16)
        here = lane == j
        mt[lax.rem(b, 3)] = jnp.where(here, row_max, mt[lax.rem(b, 3)])
        st[...] = jnp.where(here, jnp.sum(exps, axis=1, keepdims=True), st[...])
        labsum[...] += jnp.sum(jnp.where(label_mask(b, j), logits, 0.0), axis=1, keepdims=True)

    def close_block(b):
        tile_max = mt[lax.rem(b, 3)]
        row_max = jnp.max(tile_max, axis=1, keepdims=True)
        row_sum = jnp.sum(st[...] * jnp.exp((tile_max - row_max) * scale), axis=1, keepdims=True)
        packed = jnp.where(lane == 0, row_max, jnp.where(lane == 1, row_sum, labsum[...]))
        rows = packed.T[:8]
        sstat[b] = rows
        rstat[b, me] = rows
        for step in range(1, n):
            stat_send(b, peer(step)).start()

    def join_stats(b):
        for step in range(1, n):
            stat_recv(b, peer(step)).wait_recv()
        parts = [rstat[b, dev] for dev in range(n)]
        row_max = functools.reduce(jnp.maximum, [part[0:1] for part in parts])
        row_sum = sum(part[1:2] * jnp.exp((part[0:1] - row_max) * scale) for part in parts)
        row_lab = sum(part[2:3] for part in parts)
        lse = row_max * scale + jnp.log(row_sum)
        loss[...] += jnp.sum(lse - row_lab * scale)
        lse_cols = jnp.broadcast_to(lse, (128, size)).T
        cmat[...] = jnp.exp(mt[lax.rem(b, 3)] * scale - lse_cols) * scale
        gn[...] = jnp.zeros_like(gn)

    def grad_tile(b, j):
        factor = jnp.sum(jnp.where(lane == j, cmat[...], 0.0), axis=1, keepdims=True)
        exps = probs[lax.rem(b, 2), :, tile(j)].astype(jnp.float32)
        dlog = (exps * factor - jnp.where(label_mask(b, j), scale, 0.0)).astype(jnp.bfloat16)
        gn[...] += dot_nt(dlog, emb[:, tile(j)])
        det[:, tile(j)] += jnp.dot(ntr[lax.rem(b, 3)], dlog, preferred_element_type=jnp.float32)

    def wait_grad_sends(b):
        for step in range(1, n):
            grad_send(b, peer(step)).wait_send()

    def send_grads(b):
        if isinstance(b, int):
            if b >= 2:
                wait_grad_sends(b - 2)
        else:
            @pl.when(b >= 2)
            def _():
                wait_grad_sends(b - 2)
        gsend[lax.rem(b, 2)] = gn[...].astype(jnp.bfloat16)
        gr[b, me] = gn[pl.ds(pl.multiple_of(me * own, own), own), :].astype(jnp.bfloat16)
        for step in range(1, n):
            grad_send(b, peer(step)).start()

    def own_block(b):
        for step in range(1, n):
            grad_recv(b, peer(step)).wait_recv()
        grad = sum(gr[b, dev].astype(jnp.float32) for dev in range(n))
        acts = xl[own_rows(b, me), :].astype(jnp.float32)
        inv = lax.rsqrt(jnp.mean(acts * acts, axis=-1, keepdims=True) + NORM_EPS)
        normed = acts * inv
        out = inv * (grad - normed * jnp.mean(grad * normed, axis=-1, keepdims=True))
        gst[b] = out.astype(jnp.bfloat16)

        @pl.when(me < last)
        def _():
            last_send(b).start()

        @pl.when(me == last)
        def _():
            last_copy(b).start()

    det[...] = jnp.zeros_like(det)
    loss[...] = jnp.zeros_like(loss)

    @pl.loop(0, 2)
    def _(b):
        open_block(b)

        @pl.loop(0, tiles)
        def _(j):
            logits_tile(b, j)

        close_block(b)

    @pl.loop(2, blocks)
    def _(b):
        join_stats(b - 2)
        open_block(b)

        @pl.loop(0, tiles)
        def _(j):
            grad_tile(b - 2, j)
            logits_tile(b, j)

        close_block(b)

        @pl.when(b >= 3)
        def _():
            own_block(b - 3)

        send_grads(b - 2)

    @pl.loop(blocks - 2, blocks)
    def _(b):
        join_stats(b)

        @pl.loop(0, tiles)
        def _(j):
            grad_tile(b, j)

        own_block(b - 1)
        send_grads(b)

    own_block(blocks - 1)

    @pl.loop(0, blocks)
    def _(b):
        for step in range(1, n):
            stat_send(b, peer(step)).wait_send()

        @pl.when(b >= blocks - 2)
        def _():
            wait_grad_sends(b)

        @pl.when(me < last)
        def _():
            last_send(b).wait_send()

        @pl.when(me == last)
        def _():
            last_copy(b).wait()
            for dev in range(n - 1):
                last_recv(b, dev).wait_recv()


def bwd_kernel(
    n, gl, xin, h_in, dg_in, w1, w2, dw1, dw2t, gx_out,
    gin, gout, gall, hb, gb,
    f_send, g_recv, b_send, b_recv, h_sem, d_sem, o_sem,
):
    me = lax.axis_index("stage")
    last = n - 1
    size = BWD_ROWS
    count = xin.shape[0] // size
    odd = lax.rem(me, 2) == 1
    relay = jnp.logical_not(odd) & (me > 0)
    group_barrier(me, n)

    def sl(c):
        return pl.ds(pl.multiple_of(c * size, size), size)

    def h_copy(c):
        slot = lax.rem(c, 2)
        return pltpu.make_async_copy(h_in.at[sl(c)], hb.at[slot], h_sem.at[slot])

    def d_copy(c):
        slot = lax.rem(c, 2)
        return pltpu.make_async_copy(dg_in.at[sl(c)], gb.at[slot], d_sem.at[slot])

    def grad_send(c, dev):
        return remote(gout.at[sl(c)], gin.at[sl(c)], f_send.at[c], g_recv.at[c], dev)

    def bcast(src, c, which, dev):
        return remote(src.at[sl(c)], gall.at[sl(c)], b_send.at[which, c], b_recv.at[c], dev)

    h_copy(0).start()
    d_copy(0).start()
    dw1[...] = jnp.zeros_like(dw1)
    dw2t[...] = jnp.zeros_like(dw2t)

    @pl.when(me == last)
    def _():
        whole = pltpu.make_async_copy(gl, gin, o_sem.at[0])
        whole.start()
        whole.wait()

    def layer(c):
        slot = lax.rem(c, 2)

        @pl.when(c + 1 < count)
        def _():
            h_copy(c + 1).start()
            d_copy(c + 1).start()

        h_copy(c).wait()
        d_copy(c).wait()

        @pl.when(me < last)
        def _():
            grad_send(c, me).wait_recv()

        grad = gin[sl(c), :]
        grad_hidden = jnp.dot(grad, w2[...], preferred_element_type=jnp.float32)
        grad_pre = (grad_hidden * gb[slot]).astype(jnp.bfloat16)
        grad_in = grad.astype(jnp.float32) + dot_nt(grad_pre, w1[...])
        gout[sl(c), :] = grad_in.astype(jnp.bfloat16)

        @pl.when(me > 0)
        def _():
            grad_send(c, me - 1).start()

        @pl.when(me == 0)
        def _():
            bcast(gout, c, 0, 1).start()
            bcast(gout, c, 1, 2).start()
            bcast(gout, c, 2, last - 1).start()

        dw1[...] += dot_tn(xin[sl(c), :], grad_pre)
        dw2t[...] += dot_tn(grad, hb[slot])

    def relay_step(c):
        bcast(gall, c, 0, me).wait_recv()
        bcast(gall, c, 0, me + 1).start()

        @pl.when(me == 2)
        def _():
            bcast(gall, c, 1, 4).start()

    lag = jnp.where(me == 2, 6, jnp.where(me == 4, 11, 12))

    @pl.loop(0, count + 12)
    def _(i):
        @pl.when(i < count)
        def _():
            layer(i)

        @pl.when(relay & (i >= lag) & (i - lag < count))
        def _():
            relay_step(i - lag)

    @pl.when(odd)
    def _():
        @pl.loop(0, count)
        def _(c):
            bcast(gall, c, 0, me).wait_recv()

    @pl.when(me == 0)
    def _():
        whole = pltpu.make_async_copy(gout, gx_out, o_sem.at[0])
        whole.start()
        whole.wait()

    @pl.when(me > 0)
    def _():
        whole = pltpu.make_async_copy(gall, gx_out, o_sem.at[0])
        whole.start()
        whole.wait()

    @pl.loop(0, count)
    def _(c):
        @pl.when(me > 0)
        def _():
            grad_send(c, me).wait_send()

        @pl.when(jnp.logical_not(odd))
        def _():
            bcast(gall, c, 0, me).wait_send()

        @pl.when((me == 0) | (me == 2))
        def _():
            bcast(gall, c, 1, me).wait_send()

        @pl.when(me == 0)
        def _():
            bcast(gall, c, 2, me).wait_send()


def scatter_kernel(starts, ids, pos, det, gx, out, grads, acc):
    blk = pl.program_id(0)

    @pl.when(blk == 0)
    def _():
        grads[...] = gx[...].astype(jnp.float32)

    acc[...] = jnp.zeros_like(acc)
    base = blk * SCATTER_ROWS

    def add_row(k, carry):
        row = pl.ds(ids[k] - base, 1)
        acc[row, :] = acc[row, :] + grads[pl.ds(pos[k], 1), :]
        return carry

    lax.fori_loop(starts[blk], starts[blk + 1], add_row, 0)
    out[...] = det[...] + acc[...].T


def comm_params(collective_id):
    return pltpu.CompilerParams(collective_id=collective_id, has_side_effects=True, vmem_limit_bytes=VMEM_BYTES)


def solution(mesh):
    n = mesh.shape["stage"]
    bf16, f32 = jnp.bfloat16, jnp.float32
    dma = pltpu.SemaphoreType.DMA
    shape = jax.ShapeDtypeStruct

    def stage_body(token_ids, label_ids, emb_rows, w_in, w_out):
        stage_idx = lax.axis_index("stage")
        micro_count, micro_tokens = token_ids.shape
        tokens = micro_count * micro_tokens
        slice_rows, dim = emb_rows.shape
        w1, w2 = w_in[0], w_out[0].T
        ffn = w1.shape[1]
        row_start = stage_idx * slice_rows

        local_tok = token_ids.reshape(tokens) - row_start
        tok_here = (local_tok >= 0) & (local_tok < slice_rows)
        looked_up = jnp.take(emb_rows, jnp.clip(local_tok, 0, slice_rows - 1), axis=0)
        rows = jnp.where(tok_here[:, None], looked_up, 0)
        local_lab = label_ids.reshape(tokens, 1) - row_start

        keys = jnp.where(tok_here, local_tok, slice_rows)
        sorted_ids, sorted_pos = lax.sort((keys, lax.iota(jnp.int32, tokens)), num_keys=1, is_stable=False)
        edges = lax.iota(jnp.int32, slice_rows // SCATTER_ROWS + 1) * SCATTER_ROWS
        starts = jnp.sum((keys[None, :] < edges[:, None]).astype(jnp.int32), axis=1)

        size, count = FWD_ROWS, tokens // FWD_ROWS
        big = pltpu.VMEM((tokens, dim), bf16)
        xin, xl, hidden, dgelu = pl.pallas_call(
            functools.partial(fwd_kernel, n),
            name="forward",
            out_shape=[shape((tokens, dim), bf16), shape((tokens, dim), bf16), shape((tokens, ffn), bf16), shape((tokens, ffn), f32)],
            in_specs=[full_vmem()] * 3,
            out_specs=[any_space()] * 4,
            scratch_shapes=[big] * 7
            + [pltpu.VMEM((2, size, ffn), bf16), pltpu.VMEM((2, size, ffn), f32)]
            + [dma((count,))] * 6
            + [dma((3, count)), dma((count,)), dma((2,)), dma((2,)), dma((2,))],
            compiler_params=comm_params(1),
        )(rows, w1, w2)

        blocks = tokens // HEAD_ROWS
        own = HEAD_ROWS // n
        stat = pltpu.VMEM((HEAD_ROWS, 128), f32)
        det, gl, loss = pl.pallas_call(
            functools.partial(head_kernel, n),
            name="head",
            out_shape=[shape((dim, slice_rows), f32), shape((tokens, dim), bf16), shape((8, 128), f32)],
            in_specs=[full_vmem()] * 3,
            out_specs=[full_vmem(), any_space(), full_vmem()],
            scratch_shapes=[
                pltpu.VMEM((HEAD_ROWS, dim), bf16),
                pltpu.VMEM((3, dim, HEAD_ROWS), bf16),
                pltpu.VMEM((2, HEAD_ROWS, slice_rows), bf16),
                pltpu.VMEM((3, HEAD_ROWS, 128), f32),
                stat, stat, stat,
                pltpu.VMEM((HEAD_ROWS, dim), f32),
                pltpu.VMEM((2, HEAD_ROWS, dim), bf16),
                pltpu.VMEM((blocks, n, own, dim), bf16),
                pltpu.VMEM((blocks, own, dim), bf16),
                pltpu.VMEM((blocks, 8, HEAD_ROWS), f32),
                pltpu.VMEM((blocks, n, 8, HEAD_ROWS), f32),
            ]
            + [dma((blocks, n))] * 4
            + [dma((blocks,)), dma((blocks, n))],
            compiler_params=comm_params(2),
        )(xl, emb_rows.T, local_lab)

        size, count = BWD_ROWS, tokens // BWD_ROWS
        dw1, dw2t, gx = pl.pallas_call(
            functools.partial(bwd_kernel, n),
            name="backward",
            out_shape=[shape((dim, ffn), f32), shape((dim, ffn), f32), shape((tokens, dim), bf16)],
            in_specs=[any_space(), full_vmem(), any_space(), any_space(), full_vmem(), full_vmem()],
            out_specs=[full_vmem(), full_vmem(), any_space()],
            scratch_shapes=[big] * 3
            + [pltpu.VMEM((2, size, ffn), bf16), pltpu.VMEM((2, size, ffn), f32)]
            + [dma((count,))] * 2
            + [dma((3, count)), dma((count,)), dma((2,)), dma((2,)), dma((1,))],
            compiler_params=comm_params(3),
        )(gl, xin, hidden, dgelu, w1, w2)

        smem = pl.BlockSpec(memory_space=pltpu.SMEM)
        grad_emb = pl.pallas_call(
            scatter_kernel,
            name="lookup_grad",
            grid=(slice_rows // SCATTER_ROWS,),
            out_shape=shape((dim, slice_rows), f32),
            in_specs=[smem, smem, smem, pl.BlockSpec((dim, SCATTER_ROWS), lambda i: (0, i)), full_vmem()],
            out_specs=pl.BlockSpec((dim, SCATTER_ROWS), lambda i: (0, i)),
            scratch_shapes=[pltpu.VMEM((tokens, dim), f32), pltpu.VMEM((SCATTER_ROWS, dim), f32)],
            compiler_params=pltpu.CompilerParams(dimension_semantics=("arbitrary",), vmem_limit_bytes=VMEM_BYTES),
        )(starts, sorted_ids, sorted_pos, det, gx)

        mean_loss = (loss[0, :1] / tokens).astype(f32)
        return mean_loss, dw1[None], dw2t.T[None], grad_emb.T

    return jax.shard_map(
        stage_body,
        mesh=mesh,
        in_specs=(P("dp", None), P("dp", None), P("stage", None), P("stage", None, None), P("stage", None, None)),
        out_specs=(P("dp"), P(("dp", "stage"), None, None), P(("dp", "stage"), None, None), P(("dp", "stage"), None)),
        check_vma=False,
    )
```

```python
import functools

import jax
import jax.numpy as jnp
from jax import lax
from jax.experimental import pallas as pl
from jax.experimental.pallas import tpu as pltpu
from jax.sharding import PartitionSpec as P

NORM_EPS = 1e-6
MESH = pl.DeviceIdType.MESH
VMEM_BYTES = 66_000_000
FWD_ROWS = 128
BWD_ROWS = 256
HEAD_ROWS = 512
HEAD_COLS = 2048
SCATTER_ROWS = 512
GELU_K = 0.7978845608028654
GELU_C = 0.044715


def full_vmem():
    return pl.BlockSpec(memory_space=pltpu.VMEM)


def any_space():
    return pl.BlockSpec(memory_space=pl.ANY)


def remote(src, dst, send_sem, recv_sem, dev):
    return pltpu.make_async_remote_copy(
        src_ref=src, dst_ref=dst, send_sem=send_sem, recv_sem=recv_sem, device_id={"stage": dev}, device_id_type=MESH
    )


def group_barrier(me, n):
    barrier = pltpu.get_barrier_semaphore()
    for step in range(1, n):
        pl.semaphore_signal(barrier, inc=1, device_id={"stage": lax.rem(me + step, n)}, device_id_type=MESH)
    pl.semaphore_wait(barrier, n - 1)


def dot_nt(a, b):
    return lax.dot_general(a, b, (((1,), (1,)), ((), ())), preferred_element_type=jnp.float32)


def dot_tn(a, b):
    return lax.dot_general(a, b, (((0,), (0,)), ((), ())), preferred_element_type=jnp.float32)


def fwd_kernel(
    n, rows, w1, w2, xin_out, xl_out, h_out, dg_out,
    xin, xl, ea, eb, ec, es, y, hb, gb,
    e_send, ea_recv, eb_recv, ec_recv, f_send, x_recv, b_send, b_recv, h_sem, g_sem, o_sem,
):
    me = lax.axis_index("stage")
    size = FWD_ROWS
    count = rows.shape[0] // size
    last = n - 1
    odd = lax.rem(me, 2) == 1
    relay = odd & (me < last)
    group_barrier(me, n)

    def sl(c):
        return pl.ds(pl.multiple_of(c * size, size), size)

    def odd_send(c):
        return remote(rows.at[sl(c)], ea.at[sl(c)], e_send.at[c], ea_recv.at[c], me - 1)

    def even_send(c, dst, recv, dev):
        return remote(es.at[sl(c)], dst.at[sl(c)], e_send.at[c], recv.at[c], dev)

    def combine_two(c):
        even_send(c, ea, ea_recv, me).wait_recv()
        even_send(c, eb, eb_recv, me).wait_recv()
        es[sl(c), :] = rows[sl(c), :] + ea[sl(c), :] + eb[sl(c), :]
        even_send(c, eb, eb_recv, 0).start()

    def combine_four(c):
        even_send(c, ea, ea_recv, me).wait_recv()
        es[sl(c), :] = rows[sl(c), :] + ea[sl(c), :]

        @pl.when(lax.rem(c, 2) == 1)
        def _():
            even_send(c, eb, eb_recv, me).wait_recv()
            es[sl(c), :] = es[sl(c), :] + eb[sl(c), :]

        even_send(c, eb, eb_recv, 2).start()

    def combine_six(c):
        even_send(c, ea, ea_recv, me).wait_recv()
        es[sl(c), :] = rows[sl(c), :] + ea[sl(c), :]

        @pl.when(lax.rem(c, 2) == 0)
        def _():
            even_send(c, ec, ec_recv, 0).start()

        @pl.when(lax.rem(c, 2) == 1)
        def _():
            even_send(c, eb, eb_recv, 4).start()

    lead, lead_four = 8, 16

    @pl.when(odd)
    def _():
        @pl.loop(0, count)
        def _(c):
            odd_send(c).start()

    @pl.when(me == 4)
    def _():
        @pl.loop(0, lead_four)
        def _(c):
            combine_four(c)

    @pl.when(me == 6)
    def _():
        @pl.loop(0, count)
        def _(c):
            combine_six(c)

    @pl.when(me == 2)
    def _():
        @pl.loop(0, lead)
        def _(c):
            combine_two(c)

    def fwd_send(c):
        return remote(y.at[sl(c)], xin.at[sl(c)], f_send.at[c], x_recv.at[c], me + 1)

    def bcast(src, c, which, dev):
        return remote(src.at[sl(c)], xl.at[sl(c)], b_send.at[which, c], b_recv.at[c], dev)

    def h_copy(c, slot):
        return pltpu.make_async_copy(hb.at[slot], h_out.at[sl(c)], h_sem.at[slot])

    def g_copy(c, slot):
        return pltpu.make_async_copy(gb.at[slot], dg_out.at[sl(c)], g_sem.at[slot])

    def layer(c):
        slot = lax.rem(c, 2)

        @pl.when(me == 0)
        def _():
            even_send(c, ea, ea_recv, me).wait_recv()
            even_send(c, eb, eb_recv, me).wait_recv()
            xin[sl(c), :] = (rows[sl(c), :] + ea[sl(c), :]) + eb[sl(c), :]

            @pl.when(lax.rem(c, 2) == 0)
            def _():
                even_send(c, ec, ec_recv, me).wait_recv()
                xin[sl(c), :] = xin[sl(c), :] + ec[sl(c), :]

        @pl.when(me > 0)
        def _():
            remote(y.at[sl(c)], xin.at[sl(c)], f_send.at[c], x_recv.at[c], me).wait_recv()

        @pl.when(c >= 2)
        def _():
            h_copy(c - 2, slot).wait()
            g_copy(c - 2, slot).wait()

        x = xin[sl(c), :]
        pre = jnp.dot(x, w1[...], preferred_element_type=jnp.float32)
        sq = pre * pre
        th = jnp.tanh(GELU_K * (pre + GELU_C * (pre * sq)))
        cdf = 0.5 * (1.0 + th)
        hidden = (pre * cdf).astype(jnp.bfloat16)
        gb[slot] = cdf + (0.5 * pre) * (1.0 - th * th) * (GELU_K + (3.0 * GELU_K * GELU_C) * sq)
        hb[slot] = hidden
        out = x.astype(jnp.float32) + dot_nt(hidden, w2[...])
        y[sl(c), :] = out.astype(jnp.bfloat16)

        @pl.when(me < last)
        def _():
            fwd_send(c).start()

        @pl.when(me == last)
        def _():
            bcast(y, c, 0, last - 1).start()

            bcast(y, c, 1, 1).start()
            bcast(y, c, 2, last - 2).start()

        h_copy(c, slot).start()
        g_copy(c, slot).start()

    def has_next(c):
        up = lax.rem(c, 2) == 0
        return (up & (me == 1)) | (jnp.logical_not(up) & (me == last - 2))

    def relay_step(c):
        bcast(xl, c, 0, me).wait_recv()
        bcast(xl, c, 0, me - 1).start()

        @pl.when(has_next(c))
        def _():
            bcast(xl, c, 1, 3).start()

    lag = jnp.where(me == 1, 24, jnp.where(me == 3, count, 14))

    @pl.loop(0, 2 * count)
    def _(i):
        @pl.when((me == 2) & (i + lead < count))
        def _():
            combine_two(i + lead)

        @pl.when((me == 4) & (i + lead_four < count))
        def _():
            combine_four(i + lead_four)

        @pl.when(i < count)
        def _():
            layer(i)

        @pl.when(relay & (i >= lag) & (i - lag < count))
        def _():
            relay_step(i - lag)

    @pl.when(jnp.logical_not(odd))
    def _():
        @pl.loop(0, count)
        def _(c):
            bcast(xl, c, 0, me).wait_recv()

    @pl.when(me == last)
    def _():
        xl[...] = y[...]

    copy_xin = pltpu.make_async_copy(xin, xin_out, o_sem.at[0])
    copy_xl = pltpu.make_async_copy(xl, xl_out, o_sem.at[1])
    copy_xin.start()
    copy_xl.start()

    @pl.loop(0, count)
    def _(c):
        @pl.when(odd)
        def _():
            odd_send(c).wait_send()

        @pl.when(jnp.logical_not(odd) & (me > 0))
        def _():
            even_send(c, eb, eb_recv, me).wait_send()

        @pl.when(me < last)
        def _():
            fwd_send(c).wait_send()

        @pl.when(odd)
        def _():
            bcast(xl, c, 0, me).wait_send()

        @pl.when((me == last) | (relay & has_next(c)))
        def _():
            bcast(xl, c, 1, me).wait_send()

        @pl.when(me == last)
        def _():
            bcast(xl, c, 2, me).wait_send()

    for c in (count - 2, count - 1):
        h_copy(c, c % 2).wait()
        g_copy(c, c % 2).wait()
    copy_xin.wait()
    copy_xl.wait()


def head_kernel(
    n, xl, emb, lab, det, gl, loss,
    nblk, ntr, probs, mt, st, labsum, cmat, gn, gsend, gr, gst, sstat, rstat,
    s_send, s_recv, g_send, g_recv, l_send, l_recv,
):
    me = lax.axis_index("stage")
    last = n - 1
    tokens, dim = xl.shape
    slice_rows = emb.shape[1]
    size, cols = HEAD_ROWS, HEAD_COLS
    blocks, tiles = tokens // size, slice_rows // cols
    own = size // n
    scale = dim ** -0.5
    group_barrier(me, n)
    lane = lax.broadcasted_iota(jnp.int32, (size, 128), 1)

    def sl(b):
        return pl.ds(pl.multiple_of(b * size, size), size)

    def tile(j):
        return pl.ds(pl.multiple_of(j * cols, cols), cols)

    def own_rows(b, dev):
        return pl.ds(pl.multiple_of(b * size + dev * own, own), own)

    def peer(step):
        return lax.rem(me + step, n)

    def stat_send(b, dev):
        return remote(sstat.at[b], rstat.at[b, me], s_send.at[b, dev], s_recv.at[b, me], dev)

    def stat_recv(b, dev):
        return remote(sstat.at[b], rstat.at[b, dev], s_send.at[b, dev], s_recv.at[b, dev], me)

    def grad_piece(b, dev):
        return gsend.at[lax.rem(b, 2), pl.ds(pl.multiple_of(dev * own, own), own)]

    def grad_send(b, dev):
        return remote(grad_piece(b, dev), gr.at[b, me], g_send.at[b, dev], g_recv.at[b, me], dev)

    def grad_recv(b, dev):
        return remote(grad_piece(b, dev), gr.at[b, dev], g_send.at[b, dev], g_recv.at[b, dev], me)

    def last_send(b):
        return remote(gst.at[b], gl.at[own_rows(b, me)], l_send.at[b], l_recv.at[b, me], last)

    def last_recv(b, dev):
        return remote(gst.at[b], gl.at[own_rows(b, dev)], l_send.at[b], l_recv.at[b, dev], me)

    def last_copy(b):
        return pltpu.make_async_copy(gst.at[b], gl.at[own_rows(b, me)], l_send.at[b])

    def label_mask(b, j):
        ids = lax.broadcasted_iota(jnp.int32, (size, cols), 1)
        return ids == (lab[sl(b), :] - j * cols)

    def open_block(b):
        acts = xl[sl(b), :].astype(jnp.float32)
        normed = acts * lax.rsqrt(jnp.mean(acts * acts, axis=-1, keepdims=True) + NORM_EPS)
        nblk[...] = normed.astype(jnp.bfloat16)
        ntr[lax.rem(b, 3)] = normed.T.astype(jnp.bfloat16)
        mt[lax.rem(b, 3)] = jnp.full((size, 128), -jnp.inf, jnp.float32)
        st[...] = jnp.zeros((size, 128), jnp.float32)
        labsum[...] = jnp.zeros((size, 128), jnp.float32)

    def logits_tile(b, j):
        logits = jnp.dot(nblk[...], emb[:, tile(j)], preferred_element_type=jnp.float32)
        row_max = jnp.max(logits, axis=1, keepdims=True)
        exps = jnp.exp((logits - row_max) * scale)
        probs[lax.rem(b, 2), :, tile(j)] = exps.astype(jnp.bfloat16)
        here = lane == j
        mt[lax.rem(b, 3)] = jnp.where(here, row_max, mt[lax.rem(b, 3)])
        st[...] = jnp.where(here, jnp.sum(exps, axis=1, keepdims=True), st[...])
        labsum[...] += jnp.sum(jnp.where(label_mask(b, j), logits, 0.0), axis=1, keepdims=True)

    def close_block(b):
        tile_max = mt[lax.rem(b, 3)]
        row_max = jnp.max(tile_max, axis=1, keepdims=True)
        row_sum = jnp.sum(st[...] * jnp.exp((tile_max - row_max) * scale), axis=1, keepdims=True)
        packed = jnp.where(lane == 0, row_max, jnp.where(lane == 1, row_sum, labsum[...]))
        rows = packed.T[:8]
        sstat[b] = rows
        rstat[b, me] = rows
        for step in range(1, n):
            stat_send(b, peer(step)).start()

    def join_stats(b):
        for step in range(1, n):
            stat_recv(b, peer(step)).wait_recv()
        parts = [rstat[b, dev] for dev in range(n)]
        row_max = functools.reduce(jnp.maximum, [part[0:1] for part in parts])
        row_sum = sum(part[1:2] * jnp.exp((part[0:1] - row_max) * scale) for part in parts)
        row_lab = sum(part[2:3] for part in parts)
        lse = row_max * scale + jnp.log(row_sum)
        loss[...] += jnp.sum(lse - row_lab * scale)
        lse_cols = jnp.broadcast_to(lse, (128, size)).T
        cmat[...] = jnp.exp(mt[lax.rem(b, 3)] * scale - lse_cols) * scale
        gn[...] = jnp.zeros_like(gn)

    def grad_tile(b, j):
        factor = jnp.sum(jnp.where(lane == j, cmat[...], 0.0), axis=1, keepdims=True)
        exps = probs[lax.rem(b, 2), :, tile(j)].astype(jnp.float32)
        dlog = (exps * factor - jnp.where(label_mask(b, j), scale, 0.0)).astype(jnp.bfloat16)
        gn[...] += dot_nt(dlog, emb[:, tile(j)])
        det[:, tile(j)] += jnp.dot(ntr[lax.rem(b, 3)], dlog, preferred_element_type=jnp.float32)

    def wait_grad_sends(b):
        for step in range(1, n):
            grad_send(b, peer(step)).wait_send()

    def send_grads(b):
        if isinstance(b, int):
            if b >= 2:
                wait_grad_sends(b - 2)
        else:
            @pl.when(b >= 2)
            def _():
                wait_grad_sends(b - 2)
        gsend[lax.rem(b, 2)] = gn[...].astype(jnp.bfloat16)
        gr[b, me] = gn[pl.ds(pl.multiple_of(me * own, own), own), :].astype(jnp.bfloat16)
        for step in range(1, n):
            grad_send(b, peer(step)).start()

    def own_block(b):
        for step in range(1, n):
            grad_recv(b, peer(step)).wait_recv()
        grad = sum(gr[b, dev].astype(jnp.float32) for dev in range(n))
        acts = xl[own_rows(b, me), :].astype(jnp.float32)
        inv = lax.rsqrt(jnp.mean(acts * acts, axis=-1, keepdims=True) + NORM_EPS)
        normed = acts * inv
        out = inv * (grad - normed * jnp.mean(grad * normed, axis=-1, keepdims=True))
        gst[b] = out.astype(jnp.bfloat16)

        @pl.when(me < last)
        def _():
            last_send(b).start()

        @pl.when(me == last)
        def _():
            last_copy(b).start()

    det[...] = jnp.zeros_like(det)
    loss[...] = jnp.zeros_like(loss)

    @pl.loop(0, 2)
    def _(b):
        open_block(b)

        @pl.loop(0, tiles)
        def _(j):
            logits_tile(b, j)

        close_block(b)

    @pl.loop(2, blocks)
    def _(b):
        join_stats(b - 2)
        open_block(b)

        @pl.loop(0, tiles)
        def _(j):
            grad_tile(b - 2, j)
            logits_tile(b, j)

        close_block(b)

        @pl.when(b >= 3)
        def _():
            own_block(b - 3)

        send_grads(b - 2)

    @pl.loop(blocks - 2, blocks)
    def _(b):
        join_stats(b)

        @pl.loop(0, tiles)
        def _(j):
            grad_tile(b, j)

        own_block(b - 1)
        send_grads(b)

    own_block(blocks - 1)

    @pl.loop(0, blocks)
    def _(b):
        for step in range(1, n):
            stat_send(b, peer(step)).wait_send()

        @pl.when(b >= blocks - 2)
        def _():
            wait_grad_sends(b)

        @pl.when(me < last)
        def _():
            last_send(b).wait_send()

        @pl.when(me == last)
        def _():
            last_copy(b).wait()
            for dev in range(n - 1):
                last_recv(b, dev).wait_recv()


def bwd_kernel(
    n, gl, xin, h_in, dg_in, w1, w2, dw1, dw2t, gx_out,
    gin, gout, gall, hb, gb,
    f_send, g_recv, b_send, b_recv, h_sem, d_sem, o_sem,
):
    me = lax.axis_index("stage")
    last = n - 1
    size = BWD_ROWS
    count = xin.shape[0] // size
    odd = lax.rem(me, 2) == 1
    relay = jnp.logical_not(odd) & (me > 0)
    group_barrier(me, n)

    def sl(c):
        return pl.ds(pl.multiple_of(c * size, size), size)

    def h_copy(c):
        slot = lax.rem(c, 2)
        return pltpu.make_async_copy(h_in.at[sl(c)], hb.at[slot], h_sem.at[slot])

    def d_copy(c):
        slot = lax.rem(c, 2)
        return pltpu.make_async_copy(dg_in.at[sl(c)], gb.at[slot], d_sem.at[slot])

    def grad_send(c, dev):
        return remote(gout.at[sl(c)], gin.at[sl(c)], f_send.at[c], g_recv.at[c], dev)

    def bcast(src, c, which, dev):
        return remote(src.at[sl(c)], gall.at[sl(c)], b_send.at[which, c], b_recv.at[c], dev)

    h_copy(0).start()
    d_copy(0).start()
    dw1[...] = jnp.zeros_like(dw1)
    dw2t[...] = jnp.zeros_like(dw2t)

    @pl.when(me == last)
    def _():
        whole = pltpu.make_async_copy(gl, gin, o_sem.at[0])
        whole.start()
        whole.wait()

    def layer(c):
        slot = lax.rem(c, 2)

        @pl.when(c + 1 < count)
        def _():
            h_copy(c + 1).start()
            d_copy(c + 1).start()

        h_copy(c).wait()
        d_copy(c).wait()

        @pl.when(me < last)
        def _():
            grad_send(c, me).wait_recv()

        grad = gin[sl(c), :]
        grad_hidden = jnp.dot(grad, w2[...], preferred_element_type=jnp.float32)
        grad_pre = (grad_hidden * gb[slot]).astype(jnp.bfloat16)
        grad_in = grad.astype(jnp.float32) + dot_nt(grad_pre, w1[...])
        gout[sl(c), :] = grad_in.astype(jnp.bfloat16)

        @pl.when(me > 0)
        def _():
            grad_send(c, me - 1).start()

        @pl.when(me == 0)
        def _():
            bcast(gout, c, 0, 1).start()
            bcast(gout, c, 1, 2).start()
            bcast(gout, c, 2, last - 1).start()

        dw1[...] += dot_tn(xin[sl(c), :], grad_pre)
        dw2t[...] += dot_tn(grad, hb[slot])

    def relay_step(c):
        bcast(gall, c, 0, me).wait_recv()
        bcast(gall, c, 0, me + 1).start()

        @pl.when(me == 2)
        def _():
            bcast(gall, c, 1, 4).start()

    lag = jnp.where(me == 2, 6, jnp.where(me == 4, 11, 12))

    @pl.loop(0, count + 12)
    def _(i):
        @pl.when(i < count)
        def _():
            layer(i)

        @pl.when(relay & (i >= lag) & (i - lag < count))
        def _():
            relay_step(i - lag)

    @pl.when(odd)
    def _():
        @pl.loop(0, count)
        def _(c):
            bcast(gall, c, 0, me).wait_recv()

    @pl.when(me == 0)
    def _():
        whole = pltpu.make_async_copy(gout, gx_out, o_sem.at[0])
        whole.start()
        whole.wait()

    @pl.when(me > 0)
    def _():
        whole = pltpu.make_async_copy(gall, gx_out, o_sem.at[0])
        whole.start()
        whole.wait()

    @pl.loop(0, count)
    def _(c):
        @pl.when(me > 0)
        def _():
            grad_send(c, me).wait_send()

        @pl.when(jnp.logical_not(odd))
        def _():
            bcast(gall, c, 0, me).wait_send()

        @pl.when((me == 0) | (me == 2))
        def _():
            bcast(gall, c, 1, me).wait_send()

        @pl.when(me == 0)
        def _():
            bcast(gall, c, 2, me).wait_send()


def lookup_kernel(starts, ids, pos, emb, out, table, acc):
    blk = pl.program_id(0)

    @pl.when(blk == 0)
    def _():
        acc[...] = jnp.zeros_like(acc)

    table[...] = emb[...].astype(jnp.float32).T
    base = blk * SCATTER_ROWS

    def take_row(k, carry):
        acc[pl.ds(pos[k], 1), :] = table[pl.ds(ids[k] - base, 1), :]
        return carry

    lax.fori_loop(starts[blk], starts[blk + 1], take_row, 0)

    @pl.when(blk == pl.num_programs(0) - 1)
    def _():
        out[...] = acc[...].astype(jnp.bfloat16)


def scatter_kernel(starts, ids, pos, det, gx, dw1, dw2, out, dw1_out, dw2_out, grads, acc):
    blk = pl.program_id(0)
    dw1_out[...] = dw1[...]
    dw2_out[...] = dw2[...]

    @pl.when(blk == 0)
    def _():
        grads[...] = gx[...].astype(jnp.float32)

    acc[...] = jnp.zeros_like(acc)
    base = blk * SCATTER_ROWS

    def add_row(k, carry):
        row = pl.ds(ids[k] - base, 1)
        acc[row, :] = acc[row, :] + grads[pl.ds(pos[k], 1), :]
        return carry

    lax.fori_loop(starts[blk], starts[blk + 1], add_row, 0)
    out[...] = det[...] + acc[...].T


def comm_params(collective_id):
    return pltpu.CompilerParams(collective_id=collective_id, has_side_effects=True, vmem_limit_bytes=VMEM_BYTES)


def solution(mesh):
    n = mesh.shape["stage"]
    bf16, f32 = jnp.bfloat16, jnp.float32
    dma = pltpu.SemaphoreType.DMA
    shape = jax.ShapeDtypeStruct

    def stage_body(token_ids, label_ids, emb_rows, w_in, w_out):
        stage_idx = lax.axis_index("stage")
        micro_count, micro_tokens = token_ids.shape
        tokens = micro_count * micro_tokens
        slice_rows, dim = emb_rows.shape
        w1, w2 = w_in[0], w_out[0].T
        ffn = w1.shape[1]
        row_start = stage_idx * slice_rows

        local_tok = token_ids.reshape(tokens) - row_start
        tok_here = (local_tok >= 0) & (local_tok < slice_rows)
        local_lab = label_ids.reshape(tokens, 1) - row_start

        keys = jnp.where(tok_here, local_tok, slice_rows)
        sorted_ids, sorted_pos = lax.sort((keys, lax.iota(jnp.int32, tokens)), num_keys=1, is_stable=False)
        edges = lax.iota(jnp.int32, slice_rows // SCATTER_ROWS + 1) * SCATTER_ROWS
        starts = jnp.sum((keys[None, :] < edges[:, None]).astype(jnp.int32), axis=1)

        smem = pl.BlockSpec(memory_space=pltpu.SMEM)
        grid = slice_rows // SCATTER_ROWS
        emb_block = pl.BlockSpec((dim, SCATTER_ROWS), lambda i: (0, i))
        grid_params = pltpu.CompilerParams(dimension_semantics=("arbitrary",), vmem_limit_bytes=VMEM_BYTES)
        rows = pl.pallas_call(
            lookup_kernel,
            name="lookup",
            grid=(grid,),
            out_shape=shape((tokens, dim), bf16),
            in_specs=[smem, smem, smem, emb_block],
            out_specs=full_vmem(),
            scratch_shapes=[pltpu.VMEM((SCATTER_ROWS, dim), f32), pltpu.VMEM((tokens, dim), f32)],
            compiler_params=grid_params,
        )(starts, sorted_ids, sorted_pos, emb_rows.T)

        size, count = FWD_ROWS, tokens // FWD_ROWS
        big = pltpu.VMEM((tokens, dim), bf16)
        xin, xl, hidden, dgelu = pl.pallas_call(
            functools.partial(fwd_kernel, n),
            name="forward",
            out_shape=[shape((tokens, dim), bf16), shape((tokens, dim), bf16), shape((tokens, ffn), bf16), shape((tokens, ffn), f32)],
            in_specs=[full_vmem()] * 3,
            out_specs=[any_space()] * 4,
            scratch_shapes=[big] * 7
            + [pltpu.VMEM((2, size, ffn), bf16), pltpu.VMEM((2, size, ffn), f32)]
            + [dma((count,))] * 6
            + [dma((3, count)), dma((count,)), dma((2,)), dma((2,)), dma((2,))],
            compiler_params=comm_params(1),
        )(rows, w1, w2)

        blocks = tokens // HEAD_ROWS
        own = HEAD_ROWS // n
        stat = pltpu.VMEM((HEAD_ROWS, 128), f32)
        det, gl, loss = pl.pallas_call(
            functools.partial(head_kernel, n),
            name="head",
            out_shape=[shape((dim, slice_rows), f32), shape((tokens, dim), bf16), shape((8, 128), f32)],
            in_specs=[full_vmem()] * 3,
            out_specs=[full_vmem(), any_space(), full_vmem()],
            scratch_shapes=[
                pltpu.VMEM((HEAD_ROWS, dim), bf16),
                pltpu.VMEM((3, dim, HEAD_ROWS), bf16),
                pltpu.VMEM((2, HEAD_ROWS, slice_rows), bf16),
                pltpu.VMEM((3, HEAD_ROWS, 128), f32),
                stat, stat, stat,
                pltpu.VMEM((HEAD_ROWS, dim), f32),
                pltpu.VMEM((2, HEAD_ROWS, dim), bf16),
                pltpu.VMEM((blocks, n, own, dim), bf16),
                pltpu.VMEM((blocks, own, dim), bf16),
                pltpu.VMEM((blocks, 8, HEAD_ROWS), f32),
                pltpu.VMEM((blocks, n, 8, HEAD_ROWS), f32),
            ]
            + [dma((blocks, n))] * 4
            + [dma((blocks,)), dma((blocks, n))],
            compiler_params=comm_params(2),
        )(xl, emb_rows.T, local_lab)

        size, count = BWD_ROWS, tokens // BWD_ROWS
        dw1, dw2t, gx = pl.pallas_call(
            functools.partial(bwd_kernel, n),
            name="backward",
            out_shape=[shape((dim, ffn), f32), shape((dim, ffn), f32), shape((tokens, dim), bf16)],
            in_specs=[any_space(), full_vmem(), any_space(), any_space(), full_vmem(), full_vmem()],
            out_specs=[full_vmem(), full_vmem(), any_space()],
            scratch_shapes=[big] * 3
            + [pltpu.VMEM((2, size, ffn), bf16), pltpu.VMEM((2, size, ffn), f32)]
            + [dma((count,))] * 2
            + [dma((3, count)), dma((count,)), dma((2,)), dma((2,)), dma((1,))],
            compiler_params=comm_params(3),
        )(gl, xin, hidden, dgelu, w1, w2)

        dw_block = pl.BlockSpec((dim // grid, ffn), lambda i: (i, 0))
        grad_emb, dw1, dw2t = pl.pallas_call(
            scatter_kernel,
            name="lookup_grad",
            grid=(grid,),
            out_shape=[shape((dim, slice_rows), f32), shape((dim, ffn), f32), shape((dim, ffn), f32)],
            in_specs=[smem, smem, smem, emb_block, full_vmem(), dw_block, dw_block],
            out_specs=[emb_block, dw_block, dw_block],
            scratch_shapes=[pltpu.VMEM((tokens, dim), f32), pltpu.VMEM((SCATTER_ROWS, dim), f32)],
            compiler_params=grid_params,
        )(starts, sorted_ids, sorted_pos, det, gx, dw1, dw2t)

        mean_loss = (loss[0, :1] / tokens).astype(f32)
        return mean_loss, dw1[None], dw2t.T[None], grad_emb.T

    return jax.shard_map(
        stage_body,
        mesh=mesh,
        in_specs=(P("dp", None), P("dp", None), P("stage", None), P("stage", None, None), P("stage", None, None)),
        out_specs=(P("dp"), P(("dp", "stage"), None, None), P(("dp", "stage"), None, None), P(("dp", "stage"), None)),
        check_vma=False,
    )
```
